32 devices in a mesh: ga: 2 (over x), col: 16 (over z, y, core).
Axes of the slice: x: 2, y: 2, z: 4, core: 2. Of those that a mesh axis runs over, the one named last changes fastest.
Arguments:
- queries: bfloat16 [256, 32, 128], P(('ga', 'col')), parts along dimension 0, may hold values from -6 to 6
- patches: bfloat16 [64, 16, 64, 128], P(('ga', 'col')), parts along dimension 0, may hold values from -0.5 to 0.5
- top_ids: int32 [256, 32], P(('ga', 'col')), parts along dimension 0, may hold values from 0 to 31, all different within a row
Outputs:
- scores: float32 [256, 32], P('ga', 'col'), parts along dimension 0
- top_scores: float32 [256, 32], P(('ga', 'col')), parts along dimension 0
The draws below stay inside these ranges and needn't reach their ends.
There are 2 independent parts, one for each index of `ga`. The reference program is written for one: setup_inputs(seed, part) draws one part's arguments, and reference() takes and returns one part's arrays. A program takes and returns all parts, laid end to end along the dimension named above; each array names one. Nothing has to cross between parts.
Inputs may be any that keep to these rules, and one draw needn't show every extreme that they name: `top_ids`: each row names 32 different clips.
All inputs are finite; a program needn't handle non-finite values.
Results may differ from the reference program's by a relative error of at most 0.0003.
Values may be sent and summed in bfloat16 or wider, within the bound.
A program may use at most 64 MiB of HBM per device.

```python
import jax
import jax.numpy as jnp
from jax import lax

D = 128
L = 32
F = 16
P_SIZE = 64
Q = 128
CLIPS = 32
K = 32


def block_scale(stream_key, shape, split, smallest, largest):
    factor_of, own = 1.0, jax.random.fold_in(stream_key, 6)
    for dim, parts in split:
        draws = jnp.exp(jax.random.uniform(jax.random.fold_in(own, dim), (parts,), jnp.float32, smallest / len(split), largest / len(split)))
        factor_of = factor_of * jnp.repeat(draws, shape[dim] // parts).reshape([-1 if axis == dim else 1 for axis in range(len(shape))])
    return factor_of


def different_ones(stream_key, rows, count, top, lift):
    ranking = jax.random.permutation(jax.random.fold_in(stream_key, 1), count)
    favour = ranking
    for power in range(3):
        favour = favour * favour // count
    favour = favour * lift // count
    chance = jax.random.randint(jax.random.fold_in(stream_key, 2), (rows, count), 0, 4096) + favour
    sure = jax.random.permutation(jax.random.fold_in(stream_key, 3), rows)[jnp.arange(count) % rows]
    chance = jnp.where(jnp.arange(rows)[:, None] == sure[None, :], 1 << 14, chance)
    priority = chance * count + jnp.arange(count)
    return lax.top_k(priority.astype(jnp.int32), top)[1].astype(jnp.int32)


def centred(own_key, dims, spread, reach, split=(), kind=jnp.bfloat16):
    drawn = spread * jax.random.normal(own_key, dims, jnp.float32)
    if split:
        drawn = drawn * block_scale(own_key, dims, split, -0.22, 0.18)
    return jnp.clip(drawn, -reach, reach).astype(kind)


def setup_inputs(seed: int = 0, part: int = 0) -> dict:
    splits = jax.random.split(jax.random.key(seed), 4)
    own_keys = jax.random.split(jax.random.fold_in(splits[3], part), 4)
    queries = centred(own_keys[0], (Q, L, D), 1.0, 6.0, ((0, 16),))
    patches = centred(own_keys[1], (CLIPS, F, P_SIZE, D), D ** -0.5, 0.5, ((0, 16),))
    top_ids = different_ones(own_keys[2], Q, CLIPS, K, 0)
    return {"queries": queries, "patches": patches, "top_ids": top_ids}


def reference(queries, patches, top_ids):
    flat_queries = queries.reshape(-1, D).astype(jnp.float32)

    def one_clip(clip):
        block = clip.reshape(-1, D).astype(jnp.float32)
        sim = jnp.dot(flat_queries, block.T, precision=lax.Precision.HIGHEST, preferred_element_type=jnp.float32)
        best = jnp.max(sim, axis=1).reshape(Q, L)
        return jnp.sum(best, axis=1) / L

    scores = lax.map(one_clip, patches).T
    top_scores = jnp.take_along_axis(scores, top_ids, axis=1)
    return scores, top_scores
```

```python
import functools

import jax
import jax.numpy as jnp
from jax import lax
from jax.experimental import pallas as pl
from jax.experimental.pallas import tpu as pltpu
from jax.sharding import PartitionSpec as P

MESH = pl.DeviceIdType.MESH
LANES = 128
FAR = 3


def kernel(
    nz, ny, tokens, clips, rows,
    q_hbm, p_hbm, ids_hbm, scores_ref, top_ref,
    qall, pv, idv, best, got, side, mine,
    in_sem, patch_sem, z_send, far_send, y_send, recv, back_send, back_recv, side_send, side_recv, known,
):
    chips = nz * ny
    me = lax.axis_index("col")
    core = lax.rem(me, 2)
    chip = lax.div(me, 2)
    y = lax.rem(chip, ny)
    z = lax.div(chip, ny)
    partner = me + 1 - 2 * core
    _, halves, half, depth = qall.shape
    width = halves * half
    count = width // tokens
    per_clip = pv.shape[1] // clips

    def slot_of(zz, yy):
        return zz * ny + yy

    def device(slot):
        return {"col": slot * 2 + core}

    def inside(zz):
        return (zz >= 0) & (zz < nz)

    own_q = pltpu.make_async_copy(q_hbm, qall.at[chip], in_sem.at[0])
    own_q.start()
    own_p = pltpu.make_async_copy(p_hbm, pv.at[0], in_sem.at[1])
    own_p.start()
    own_i = pltpu.make_async_copy(ids_hbm, idv, in_sem.at[2])
    own_i.start()

    barrier = pltpu.get_barrier_semaphore()
    pl.semaphore_signal(barrier, inc=1, device_id={"col": partner}, device_id_type=MESH)
    greeted = 1
    if ny == 2:
        pl.semaphore_signal(barrier, inc=1, device_id=device(slot_of(z, 1 - y)), device_id_type=MESH)
        greeted = 2
    for step in (1, -1):
        there = inside(z + step)

        @pl.when(there)
        def _():
            pl.semaphore_signal(barrier, inc=1, device_id=device(slot_of(z + step, y)), device_id_type=MESH)

        greeted = greeted + jnp.where(there, 1, 0)
    pl.semaphore_wait(barrier, greeted)

    def piece(slot, h, target, sem):
        return pltpu.make_async_remote_copy(
            src_ref=qall.at[slot, h], dst_ref=qall.at[slot, h], send_sem=sem, recv_sem=recv.at[slot, h],
            device_id=target, device_id_type=MESH,
        )

    def z_copy(slot, h, way):
        return piece(slot, h, device(slot_of(z + way, y)), z_send.at[(1 - way) // 2, slot, h])

    def far_copy(row, h, way):
        slot = slot_of(z, y if row == 0 else 1 - y)
        return piece(slot, h, device(slot_of(z + FAR * way, y)), far_send.at[row, (1 - way) // 2, h])

    def y_copy(slot, h):
        return piece(slot, h, device(slot_of(z, 1 - y)), y_send.at[slot, h])

    def back_copy(slot, origin, target):
        return pltpu.make_async_remote_copy(
            src_ref=best.at[slot], dst_ref=got.at[origin], send_sem=back_send.at[slot], recv_sem=back_recv.at[origin],
            device_id=target, device_id_type=MESH,
        )

    def side_copy(slot):
        return pltpu.make_async_remote_copy(
            src_ref=best.at[slot], dst_ref=side.at[slot], send_sem=side_send.at[slot], recv_sem=side_recv.at[slot],
            device_id={"col": partner}, device_id_type=MESH,
        )

    patch_copy = pltpu.make_async_remote_copy(
        src_ref=pv.at[0], dst_ref=pv.at[1], send_sem=patch_sem.at[0], recv_sem=patch_sem.at[1],
        device_id={"col": partner}, device_id_type=MESH,
    )

    def arrived(slot, h):
        piece(slot, h, {"col": partner}, y_send.at[slot, h]).wait_recv()

    def compute(slot, sides=(0, 1)):
        q = qall[slot].reshape(width, depth)
        for i in sides:
            for j in range(clips):
                top = None
                for r in range(per_clip // rows):
                    sim = lax.dot_general(
                        pv[i, pl.ds(j * per_clip + r * rows, rows), :], q, (((1,), (1,)), ((), ())),
                        preferred_element_type=jnp.float32,
                    )
                    part = jnp.max(sim.reshape(rows // 8, 8, width), axis=0)
                    top = part if top is None else jnp.maximum(top, part)
                best[slot, pl.ds(i * clips + j, 1), :] = jnp.max(top, axis=0, keepdims=True)

    def done(slot):
        back_copy(slot, chip, device(slot)).start()
        side_copy(slot).start()

    own_q.wait()
    for h in range(halves):
        for way in (1, -1):

            @pl.when(inside(z + way))
            def _():
                z_copy(chip, h, way).start()

        if ny == 2:
            y_copy(chip, h).start()
    own_p.wait()
    patch_copy.start()
    for stage in range(1, FAR):
        for way in (1, -1):

            @pl.when(inside(z + way) & inside(z - way * stage))
            def _():
                pl.semaphore_signal(
                    known.at[(1 - way) // 2, stage - 1], inc=1,
                    device_id=device(slot_of(z + way, y)), device_id_type=MESH,
                )

        for way in (1, -1):

            @pl.when(inside(z - way * (stage + 1)))
            def _():
                pl.semaphore_wait(known.at[(1 - way) // 2, stage - 1], 1)

    for h in range(halves):
        for way in (1, -1):

            @pl.when(inside(z + FAR * way))
            def _():
                far_copy(0, h, way).start()

    compute(chip, (0,))

    def onward(z_from, d, way):
        return inside(z_from) & inside(z + way) & (d + 1 != FAR)

    def step(d, carry):
        for way in (1, -1):
            z_from = z - way * d
            slot = slot_of(z_from, y)

            @pl.when(inside(z_from))
            def _():
                for h in range(halves):
                    arrived(slot, h)

                    @pl.when(onward(z_from, d, way))
                    def _():
                        z_copy(slot, h, way).start()

                    if ny == 2:

                        @pl.when(d != FAR)
                        def _():
                            y_copy(slot, h).start()

        @pl.when(d == 1)
        def _():
            if ny == 2:
                for h in range(halves):
                    arrived(slot_of(z, 1 - y), h)
                    for way in (1, -1):

                        @pl.when(inside(z + FAR * way))
                        def _():
                            far_copy(1, h, way).start()

            patch_copy.wait_recv()
            compute(chip, (1,))
            side_copy(chip).start()

        for way in (1, -1):
            z_from = z - way * d
            slot = slot_of(z_from, y)

            @pl.when(inside(z_from) & (d < nz))
            def _():
                compute(slot)
                done(slot)

        if ny == 2:
            late(d - 1)
        return carry

    def late(d):
        for way in (1, -1):
            z_from = z - way * d
            slot = slot_of(z_from, 1 - y)

            @pl.when(inside(z_from) & ((d > 0) | (way > 0)))
            def _():
                @pl.when(d > 0)
                def _():
                    for h in range(halves):
                        arrived(slot, h)

                compute(slot)
                done(slot)

    lax.fori_loop(1, nz + (ny - 1), step, 0)

    total = 2 * chips * count
    token = lax.broadcasted_iota(jnp.int32, (width, total), 0)
    lane = lax.broadcasted_iota(jnp.int32, (width, total), 1)
    pick = jnp.where(lax.div(token, tokens) == lax.rem(lane, count), 1.0, 0.0).astype(jnp.float32)
    row_of = lax.broadcasted_iota(jnp.int32, (chips, total), 0)
    lane_of = lax.div(lax.broadcasted_iota(jnp.int32, (chips, total), 1), count)
    here = row_of == lax.div(lane_of, 2)
    ours = lax.rem(lane_of, 2) == core

    def take(i, carry):
        side_copy(i).wait_recv()
        return carry

    lax.fori_loop(0, chips, take, 0)
    for j in range(clips):
        near = jnp.dot(best[:, j, :], pick, precision=lax.Precision.HIGHEST, preferred_element_type=jnp.float32)
        far = jnp.dot(side[:, clips + j, :], pick, precision=lax.Precision.HIGHEST, preferred_element_type=jnp.float32)
        kept_sums = jnp.where(here, jnp.where(ours, near, far), 0.0)
        scores_ref[pl.ds(j, 1), :] = jnp.sum(kept_sums, axis=0, keepdims=True) / tokens

    own_i.wait()
    mine[...] = jnp.zeros_like(mine)
    got[chip] = best[chip]
    ids = idv[...]
    both = 2 * clips
    swapped = lax.rem(lax.rem(lax.div(ids, clips), 2) + core, 2)
    place = (swapped * clips + lax.rem(ids, clips)) * chips + lax.div(ids, both)
    kept = ids.shape[1]
    padded = jnp.concatenate([place, jnp.zeros((count, LANES - kept), jnp.int32)], axis=1)
    q_of = lax.broadcasted_iota(jnp.int32, (count, width), 0)
    t_of = lax.broadcasted_iota(jnp.int32, (count, width), 1)
    select = jnp.where(lax.div(t_of, tokens) == q_of, 1.0, 0.0).astype(jnp.float32)

    def collect(i, carry):
        origin = lax.rem(chip + i, chips)
        back_copy(origin, origin, {"col": partner}).wait_recv()
        return carry

    lax.fori_loop(1, chips, collect, 0)
    for j in range(both):
        mine[:, pl.ds(j * chips, chips)] = lax.dot_general(
            select, got[:, j, :], (((1,), (1,)), ((), ())),
            precision=lax.Precision.HIGHEST, preferred_element_type=jnp.float32,
        ) / tokens
    chosen = jnp.zeros((count, LANES), jnp.float32)
    for w in range(mine.shape[1] // LANES):
        local = jnp.take_along_axis(mine[:, pl.ds(w * LANES, LANES)], lax.rem(padded, LANES), axis=1)
        chosen = jnp.where(lax.div(padded, LANES) == w, local, chosen)
    top_ref[...] = chosen[:, :kept]

    patch_copy.wait_send()
    for h in range(halves):
        for way in (1, -1):

            @pl.when(inside(z + FAR * way))
            def _():
                for row in range(ny):
                    far_copy(row, h, way).wait_send()

    def left(d, carry):
        for way in (1, -1):
            z_from = z - way * d
            slot = slot_of(z_from, y)
            for h in range(halves):

                @pl.when(onward(z_from, d, way))
                def _():
                    z_copy(slot, h, way).wait_send()

                if ny == 2:

                    @pl.when(inside(z_from) & ((d > 0) | (way > 0)) & (d != FAR))
                    def _():
                        y_copy(slot, h).wait_send()

        return carry

    lax.fori_loop(0, nz, left, 0)

    def left_back(i, carry):
        slot = lax.rem(chip + i, chips)

        @pl.when(i > 0)
        def _():
            back_copy(slot, chip, device(slot)).wait_send()

        side_copy(slot).wait_send()
        return carry

    lax.fori_loop(0, chips, left_back, 0)


def across_y(mesh):
    line = mesh.devices[0]
    if len(line) % 4 or not hasattr(line[0], "coords"):
        return 1
    return 2 if len({d.coords[1] for d in line}) == 2 else 1


def solution(mesh):
    n = mesh.shape["col"]
    ny = across_y(mesh)
    nz = n // (2 * ny)

    def per_device(queries, patches, top_ids):
        clips, frames, per_frame, depth = patches.shape
        count, tokens, _ = queries.shape
        width = count * tokens
        per_clip = frames * per_frame
        kept = top_ids.shape[1]
        rows = 256
        halves = 1
        chips = nz * ny
        wide = -(-(clips * n) // LANES) * LANES
        anywhere = pl.BlockSpec(memory_space=pl.ANY)
        vmem = pl.BlockSpec(memory_space=pltpu.VMEM)
        scores, top = pl.pallas_call(
            functools.partial(kernel, nz, ny, tokens, clips, rows),
            out_shape=(
                pltpu.VMEM((clips, n * count), jnp.float32),
                pltpu.VMEM((count, kept), jnp.float32),
            ),
            in_specs=[anywhere] * 3,
            out_specs=(vmem, vmem),
            scratch_shapes=[
                pltpu.VMEM((chips, halves, width // halves, depth), jnp.bfloat16),
                pltpu.VMEM((2, clips * per_clip, depth), jnp.bfloat16),
                pltpu.VMEM((count, kept), jnp.int32),
                pltpu.VMEM((chips, 2 * clips, width), jnp.float32),
                pltpu.VMEM((chips, 2 * clips, width), jnp.float32),
                pltpu.VMEM((chips, 2 * clips, width), jnp.float32),
                pltpu.VMEM((count, wide), jnp.float32),
                pltpu.SemaphoreType.DMA((3,)),
                pltpu.SemaphoreType.DMA((2,)),
                pltpu.SemaphoreType.DMA((2, chips, halves)),
                pltpu.SemaphoreType.DMA((ny, 2, halves)),
                pltpu.SemaphoreType.DMA((chips, halves)),
                pltpu.SemaphoreType.DMA((chips, halves)),
                pltpu.SemaphoreType.DMA((chips,)),
                pltpu.SemaphoreType.DMA((chips,)),
                pltpu.SemaphoreType.DMA((chips,)),
                pltpu.SemaphoreType.DMA((chips,)),
                pltpu.SemaphoreType.REGULAR((2, FAR - 1)),
            ],
            compiler_params=pltpu.CompilerParams(collective_id=0, has_side_effects=True),
        )(
            queries.reshape(halves, width // halves, depth),
            patches.reshape(clips * per_clip, depth),
            top_ids,
        )
        def out_kernel(a, b, c, d, sem):
            x = pltpu.make_async_copy(a, c, sem.at[0])
            y = pltpu.make_async_copy(b, d, sem.at[1])
            x.start()
            y.start()
            x.wait()
            y.wait()

        scores, top = pl.pallas_call(
            out_kernel,
            out_shape=(
                jax.ShapeDtypeStruct((clips, n * count), jnp.float32),
                jax.ShapeDtypeStruct((count, kept), jnp.float32),
            ),
            in_specs=[vmem, vmem],
            out_specs=(anywhere, anywhere),
            scratch_shapes=[pltpu.SemaphoreType.DMA((2,))],
        )(pltpu.with_memory_space_constraint(scores, pltpu.VMEM), pltpu.with_memory_space_constraint(top, pltpu.VMEM))
        return scores.T, top

    return jax.shard_map(
        per_device,
        mesh=mesh,
        in_specs=(
            P(("ga", "col"), None, None),
            P(("ga", "col"), None, None, None),
            P(("ga", "col"), None),
        ),
        out_specs=(P("ga", "col"), P(("ga", "col"), None)),
        check_vma=False,
    )
```
